128 devices in a mesh: row: 16 (over z_lo, x, core), col: 4 (over y), layer: 2 (over z_hi).
Axes of the slice: x: 4, y: 4, z: 4 (z_hi: 2, z_lo: 2; z = z_hi * 2 + z_lo), core: 2. Of those that a mesh axis runs over, the one named last changes fastest.
Arguments:
- attn_values: bfloat16 [8192, 8192], P('row', ('layer', 'col')), may hold values from -6 to 6
- out_weight: bfloat16 [8192, 8192], P(('layer', 'row'), 'col'), may hold values from -0.125 to 0.125
Outputs:
- projected: bfloat16 [8192, 8192], P('row', ('col', 'layer'))
The draws below stay inside these ranges and needn't reach their ends.
All inputs are finite; a program needn't handle non-finite values.
Results may differ from the reference program's by a relative error of at most 0.001.
Values may be sent and summed in bfloat16 or wider, within the bound.
No kernel may reach another device: no remote copies, remote signals or barrier semaphores. Data moves between devices by JAX's collectives and lax.ppermute only.
A program may use at most 128 MiB of HBM per device.

```python
import jax
import jax.numpy as jnp
from jax import lax

D = 8192
TOK_DEV = 512
TOKENS = 8192
N_ROW = 16


def with_spikes(entries, own_key, source, target, parts, factor):
    owner, partner = [(jnp.arange(entries.shape[axis_at]) // (entries.shape[axis_at] // parts)).reshape([-1 if axis == axis_at else 1 for axis in range(entries.ndim)]) for axis_at in (source, target)]
    chosen = jax.random.permutation(own_key, parts)[partner]
    strong = (owner == chosen) | (owner == (partner + parts // 2) % parts)
    return jnp.where(strong, factor * entries, entries)


def levels(stream_key, extent, pieces, low, high):
    loudness, own = 1.0, jax.random.fold_in(stream_key, 6)
    for axis_at, blocks in pieces:
        heights = jnp.exp(jax.random.uniform(jax.random.fold_in(own, axis_at), (blocks,), jnp.float32, low / len(pieces), high / len(pieces)))
        loudness = loudness * jnp.repeat(heights, extent[axis_at] // blocks).reshape([-1 if axis == axis_at else 1 for axis in range(len(extent))])
    return loudness


def noise(rng, dims, spread, bound, cuts=(), kind=jnp.bfloat16):
    loudness = levels(rng, dims, cuts, -0.22, 0.18) if cuts else 1.0
    entries = jax.random.normal(rng, dims, jnp.float32) * spread * loudness
    return jnp.minimum(jnp.maximum(entries, -bound), bound).astype(kind)


def bell_draw_with(rng, dims, spread, bound, shards, heavy, held_as=jnp.bfloat16):
    array = spread * jax.random.normal(rng, dims, jnp.float32)
    if shards:
        array = array * levels(rng, dims, shards, -0.22, 0.18)
    return jnp.clip(with_spikes(array, jax.random.fold_in(rng, 3), *heavy), -bound, bound).astype(held_as)


def setup_inputs(seed: int = 0) -> dict:
    seeds = jax.random.split(jax.random.key(seed), 3)
    return {
        "attn_values": noise(seeds[0], (TOKENS, D), 1.0, 6.0, ((0, 16), (1, 8))),
        "out_weight": bell_draw_with(seeds[1], (D, D), D ** -0.5, 0.125, ((0, 32), (1, 4)), (0, 1, 32, 2.75)),
    }


def reference(attn_values, out_weight):
    token_blocks = attn_values.reshape(N_ROW, TOK_DEV, D)
    half_depth = D // 2

    def project(block):
        lower_part = jnp.dot(block[:, :half_depth], out_weight[:half_depth], preferred_element_type=jnp.float32)
        upper_part = jnp.dot(block[:, half_depth:], out_weight[half_depth:], preferred_element_type=jnp.float32)
        return (lower_part + upper_part).astype(jnp.bfloat16)

    return lax.map(project, token_blocks).reshape(TOK_DEV * N_ROW, D)
```

```python
import jax
import jax.numpy as jnp
from jax import lax
from jax.experimental import pallas as pl
from jax.experimental.pallas import tpu as pltpu
from jax.sharding import PartitionSpec as P

AXES = ("row", "col", "layer")


def device_at(x, y, z, core):
    x, y, z = x % 4, y % 4, z % 4
    return (((z % 2) * 8 + x * 2 + core) * 4 + y) * 2 + z // 2


def pairs(move):
    return [
        (device_at(x, y, z, core), device_at(*move(x, y, z, core)))
        for x in range(4)
        for y in range(4)
        for z in range(4)
        for core in range(2)
    ]


def z_of(hi, lo):
    return hi * 2 + lo


MOVES = {
    "x+": pairs(lambda x, y, z, c: (x + 1, y, z, c)),
    "x-": pairs(lambda x, y, z, c: (x - 1, y, z, c)),
    "y+": pairs(lambda x, y, z, c: (x, y + 1, z, c)),
    "y-": pairs(lambda x, y, z, c: (x, y - 1, z, c)),
    "near": pairs(lambda x, y, z, c: (x, y, z_of(z // 2, 1 - z % 2), c)),
    "far": pairs(lambda x, y, z, c: (x, y, z_of(1 - z // 2, z % 2), c)),
    "diag": pairs(lambda x, y, z, c: (x, y, z_of(1 - z // 2, 1 - z % 2), c)),
    "core": pairs(lambda x, y, z, c: (x, y, z, 1 - c)),
}


def send(value, move):
    return lax.ppermute(value, AXES, MOVES[move])


def ring(block, axis):
    half = block.shape[0] // 2
    below = send(block, axis + "+")
    above = send(block, axis + "-")
    top = send(below[:half], axis + "+")
    bottom = send(above[half:], axis + "-")
    return [block, below, above, top, bottom]


def product_kernel(where, *refs, has_sum):
    a_parts, w_parts, rest = refs[:5], refs[5:25], refs[25:]
    if has_sum:
        earlier, out, a_all, w_all = rest
    else:
        out, a_all, w_all = rest
    x, core, z_lo, y = where[0], where[1], where[2], where[3]
    for ref, turn, start in zip(a_parts, (0, 3, 1, 2, 2), (0, 0, 0, 0, 256)):
        at = pl.multiple_of(((y + turn) % 4) * 1024, 1024)
        a_all[start : start + ref.shape[0], pl.ds(at, 1024)] = ref[...]
    for group in range(4):
        lo = (z_lo + group // 2) % 2
        c = (core + group % 2) % 2
        for ref, turn, start in zip(
            w_parts[group * 5 : group * 5 + 5], (0, 3, 1, 2, 2), (0, 0, 0, 0, 128)
        ):
            at = pl.multiple_of((lo * 8 + ((x + turn) % 4) * 2 + c) * 256 + start, 128)
            w_all[pl.ds(at, ref.shape[0]), :] = ref[...]
    for n in range(0, 1024, 256):
        tile = jnp.dot(a_all[...], w_all[:, n : n + 256], preferred_element_type=jnp.float32)
        if has_sum:
            tile = tile + earlier[:, n : n + 256]
        out[:, n : n + 256] = tile.astype(out.dtype)


def product(where, a_parts, w_parts, earlier, dtype):
    operands = [where, *a_parts, *w_parts] + ([] if earlier is None else [earlier])
    vmem = pl.BlockSpec(memory_space=pltpu.VMEM)

    def kernel(*refs):
        product_kernel(*refs, has_sum=earlier is not None)

    return pl.pallas_call(
        kernel,
        out_shape=jax.ShapeDtypeStruct((512, 1024), dtype),
        in_specs=[pl.BlockSpec(memory_space=pltpu.SMEM)] + [vmem] * (len(operands) - 1),
        out_specs=vmem,
        scratch_shapes=[
            pltpu.VMEM((512, 4096), jnp.bfloat16),
            pltpu.VMEM((4096, 1024), jnp.bfloat16),
        ],
        compiler_params=pltpu.CompilerParams(vmem_limit_bytes=40 * 1024 * 1024),
        cost_estimate=pl.CostEstimate(
            flops=2 * 512 * 4096 * 1024, bytes_accessed=16 * 1024 * 1024, transcendentals=0
        ),
    )(*operands)


def shards(a, w):
    row, y, layer = (lax.axis_index(n) for n in AXES)
    where = jnp.stack([(row // 2) % 4, row % 2, row // 8, y]).astype(jnp.int32)
    mine = lax.dynamic_slice_in_dim(w, layer * 1024, 1024, 1)
    theirs = lax.dynamic_slice_in_dim(w, (1 - layer) * 1024, 1024, 1)
    a_own = ring(a, "y")
    w_own = ring(mine, "x")
    w_near = ring(send(mine, "near"), "x")
    w_diag_in = send(theirs, "diag")
    a_far_in = send(a, "far")
    w_far_in = send(theirs, "far")
    a_far = ring(a_far_in, "y")
    w_diag = ring(w_diag_in, "x")
    w_far = ring(w_far_in, "x")

    def both(parts):
        return parts + [send(p, "core") for p in parts]

    first = product(where, a_own, both(w_own) + both(w_near), None, jnp.float32)
    return product(where, a_far, both(w_far) + both(w_diag), first, jnp.bfloat16)


def solution(mesh):
    in_specs = (P("row", ("layer", "col")), P(("layer", "row"), "col"))
    out_specs = P("row", ("col", "layer"))
    return jax.shard_map(shards, mesh=mesh, in_specs=in_specs, out_specs=out_specs, check_vma=False)
```
